16 devices in a mesh: dp: 2 (over y, z), sp: 8 (over x, core).
Axes of the slice: x: 4, y: 2, z: 1, core: 2. Of those that a mesh axis runs over, the one named last changes fastest.
The devices are a block of a 4x4x8 slice.
Arguments:
- x_in: bfloat16 [12, 1024, 1024], P('dp', 'sp'), parts along dimension 0
- positions: int32 [2048], P(('dp', 'sp')), parts along dimension 0
- d_out: bfloat16 [12, 1024, 1024], P('dp', 'sp'), parts along dimension 0
- w_query: bfloat16 [2, 1024, 16, 64], replicated
- w_key: bfloat16 [2, 1024, 16, 64], replicated
- w_value: bfloat16 [2, 1024, 16, 64], replicated
- w_attn_out: bfloat16 [2, 16, 64, 1024], replicated
- w_up: bfloat16 [2, 1024, 4096], replicated
- w_down: bfloat16 [2, 4096, 1024], replicated
- g_attn: float32 [2, 1024], replicated
- g_mlp: float32 [2, 1024], replicated
- learn_rate: float32 [], replicated
Outputs:
- output 1: bfloat16 [12, 1024, 1024], P('dp', 'sp'), parts along dimension 0
- output 2: bfloat16 [12, 1024, 1024], P('dp', 'sp'), parts along dimension 0
- output 3: bfloat16 [4, 1024, 16, 64], P('dp'), parts along dimension 0
- output 4: bfloat16 [4, 1024, 16, 64], P('dp'), parts along dimension 0
- output 5: bfloat16 [4, 1024, 16, 64], P('dp'), parts along dimension 0
- output 6: bfloat16 [4, 16, 64, 1024], P('dp'), parts along dimension 0
- output 7: bfloat16 [4, 1024, 4096], P('dp'), parts along dimension 0
- output 8: bfloat16 [4, 4096, 1024], P('dp'), parts along dimension 0
There are 2 independent parts. The reference program is written for one: setup_inputs(seed, part) draws one part's arguments, and reference() takes and returns one part's arrays. A program takes and returns all parts, laid end to end along the dimension named above; an argument that names none is the same for every part.
All inputs are finite; a program needn't handle non-finite values.
Results may differ from the reference program's by a relative error of at most 0.02.
Values are sent between devices in bfloat16 or wider.
A program may use at most 768 MiB of HBM per device.

```python
import math
import jax
import jax.numpy as jnp
from jax import lax

BATCH = 6
SEQ_LEN = 1024
D_MODEL = 1024
HEADS = 16
KV_HEADS = 16
HEAD_DIM = 64
FF_DIM = 4096
LAYERS = 2
EPSILON = 1e-5
ROPE_BASE = 10000.0


def setup_inputs(seed: int = 0, part: int = 0) -> dict:
    base_key = jax.random.key(seed)
    part_key = jax.random.fold_in(base_key, part)
    key_x, key_pos, key_dy = jax.random.split(part_key, 3)
    shared = jax.random.split(base_key, 9)
    sharp = (math.log(SEQ_LEN) / 2.0) ** 0.25
    width_q = D_MODEL ** -0.5 * sharp

    def normal(key, dims, std):
        return (jax.random.normal(key, dims, jnp.float32) * std).astype(jnp.bfloat16)

    steps = jax.random.randint(key_pos, (SEQ_LEN,), 1, 3)
    positions = (jnp.cumsum(steps) - steps[0]).astype(jnp.int32)
    learn_rate = jax.random.uniform(shared[8], (), jnp.float32, 0.5, 1.5) * 0.2 / math.sqrt(BATCH * SEQ_LEN * D_MODEL)
    return {
        'x_in': normal(key_x, (BATCH, SEQ_LEN, D_MODEL), 1.0),
        'positions': positions,
        'd_out': normal(key_dy, (BATCH, SEQ_LEN, D_MODEL), 1.0),
        'w_query': normal(shared[0], (LAYERS, D_MODEL, HEADS, HEAD_DIM), width_q),
        'w_key': normal(shared[1], (LAYERS, D_MODEL, KV_HEADS, HEAD_DIM), width_q),
        'w_value': normal(shared[2], (LAYERS, D_MODEL, KV_HEADS, HEAD_DIM), D_MODEL ** -0.5),
        'w_attn_out': normal(shared[3], (LAYERS, HEADS, HEAD_DIM, D_MODEL), (HEADS * HEAD_DIM) ** -0.5 * SEQ_LEN ** 0.15),
        'w_up': normal(shared[4], (LAYERS, D_MODEL, FF_DIM), D_MODEL ** -0.5),
        'w_down': normal(shared[5], (LAYERS, FF_DIM, D_MODEL), FF_DIM ** -0.5),
        'g_attn': 1.0 + 0.3 * jax.random.normal(shared[6], (LAYERS, D_MODEL), jnp.float32),
        'g_mlp': 1.0 + 0.3 * jax.random.normal(shared[7], (LAYERS, D_MODEL), jnp.float32),
        'learn_rate': learn_rate,
    }


def contract(form, left, right):
    return jnp.einsum(form, left.astype(jnp.float32), right.astype(jnp.float32))


def gelu_tanh(value):
    return jax.nn.gelu(value, approximate=True)


def rms_norm(act, gain):
    wide = act.astype(jnp.float32)
    inv_rms = lax.rsqrt(jnp.mean(wide * wide, axis=-1, keepdims=True) + EPSILON)
    return (wide * inv_rms * gain).astype(jnp.bfloat16), inv_rms


def rms_norm_grad(act, inv_rms, gain, d_norm):
    wide = act.astype(jnp.float32)
    d_gain = d_norm * gain
    return inv_rms * d_gain - wide * inv_rms ** 3 * jnp.mean(d_gain * wide, axis=-1, keepdims=True)


def rotary(heads, positions, sign):
    half_dim = heads.shape[-1] // 2
    inv_freq = ROPE_BASE ** (-2.0 * jnp.arange(half_dim, dtype=jnp.float32) / heads.shape[-1])
    angle = positions.astype(jnp.float32)[..., None] * inv_freq
    cosine = jnp.cos(angle)[..., None, :]
    sine = sign * jnp.sin(angle)[..., None, :]
    first = heads[..., :half_dim]
    second = heads[..., half_dim:]
    return jnp.concatenate([first * cosine - second * sine, second * cosine + first * sine], axis=-1)


def causal_scores(q_heads, k_heads):
    scores = contract('bqgre,bkge->bgrqk', q_heads, k_heads) * q_heads.shape[-1] ** -0.5
    allowed = jnp.arange(q_heads.shape[1])[:, None] >= jnp.arange(k_heads.shape[1])[None, :]
    return jnp.where(allowed, scores, -1e30)


def attn_forward(q_heads, k_heads, v_heads):
    scores = causal_scores(q_heads, k_heads)
    row_max = jnp.max(scores, axis=-1, keepdims=True)
    shifted_exp = jnp.exp(scores - row_max)
    row_sum = jnp.sum(shifted_exp, axis=-1, keepdims=True)
    probs_low = (shifted_exp / row_sum).astype(jnp.bfloat16)
    attn_out = contract('bgrqk,bkge->bqgre', probs_low, v_heads).astype(jnp.bfloat16)
    return attn_out, (row_max + jnp.log(row_sum))[..., 0]


def attn_backward(q_heads, k_heads, v_heads, out_heads, log_sum, d_heads):
    probs = jnp.exp(causal_scores(q_heads, k_heads) - log_sum[..., None])
    probs_low = probs.astype(jnp.bfloat16)
    d_values = contract('bgrqk,bqgre->bkge', probs_low, d_heads)
    d_probs = contract('bqgre,bkge->bgrqk', d_heads, v_heads)
    delta = contract('bqgre,bqgre->bgrq', d_heads, out_heads)
    d_scores = (probs * (d_probs - delta[..., None]) * q_heads.shape[-1] ** -0.5).astype(jnp.bfloat16)
    d_query = contract('bgrqk,bkge->bqgre', d_scores, k_heads)
    d_keys = contract('bgrqk,bqgre->bkge', d_scores, q_heads)
    return d_query, d_keys, d_values


def grouped_attention(q_group, keys, values):
    def one_group(item):
        q_item, k_item, v_item = item
        return attn_forward(q_item[:, :, None], k_item[:, :, None], v_item[:, :, None])
    outs, log_sum = lax.map(one_group, (jnp.moveaxis(q_group, 2, 0), jnp.moveaxis(keys, 2, 0), jnp.moveaxis(values, 2, 0)))
    return jnp.moveaxis(outs[:, :, :, 0], 0, 2), log_sum


def grouped_attention_grad(q_group, keys, values, attn_out, log_sum, d_group):
    def one_group(item):
        q_item, k_item, v_item, o_item, lse_item, d_item = item
        return attn_backward(q_item[:, :, None], k_item[:, :, None], v_item[:, :, None], o_item[:, :, None], lse_item, d_item[:, :, None])
    d_query, d_keys, d_values = lax.map(one_group, (jnp.moveaxis(q_group, 2, 0), jnp.moveaxis(keys, 2, 0), jnp.moveaxis(values, 2, 0), jnp.moveaxis(attn_out, 2, 0), log_sum, jnp.moveaxis(d_group, 2, 0)))
    return (jnp.moveaxis(d_query[:, :, :, 0], 0, 2), jnp.moveaxis(d_keys[:, :, :, 0], 0, 2), jnp.moveaxis(d_values[:, :, :, 0], 0, 2))


def reference(x_in, positions, d_out, w_query, w_key, w_value, w_attn_out, w_up, w_down, g_attn, g_mlp, learn_rate):
    weights = (w_query, w_key, w_value, w_attn_out, w_up, w_down)
    act = x_in
    stashes = []
    for layer in range(LAYERS):
        norm_attn, inv_attn = rms_norm(act, g_attn[layer])
        query = rotary(contract('bsd,dhe->bshe', norm_attn, w_query[layer]), positions, 1.0).astype(jnp.bfloat16)
        keys = rotary(contract('bsd,dhe->bshe', norm_attn, w_key[layer]), positions, 1.0).astype(jnp.bfloat16)
        values = contract('bsd,dhe->bshe', norm_attn, w_value[layer]).astype(jnp.bfloat16)
        q_group = query.reshape(query.shape[0], query.shape[1], keys.shape[2], -1, query.shape[3])
        attn_out, log_sum = grouped_attention(q_group, keys, values)
        mixed = attn_out.reshape(query.shape)
        hidden = (act.astype(jnp.float32) + contract('bshe,hed->bsd', mixed, w_attn_out[layer])).astype(jnp.bfloat16)
        norm_mlp, inv_mlp = rms_norm(hidden, g_mlp[layer])
        pre_act = contract('bsd,df->bsf', norm_mlp, w_up[layer])
        gelu_out = gelu_tanh(pre_act).astype(jnp.bfloat16)
        stashes.append((act, norm_attn, inv_attn, q_group, keys, values, attn_out, log_sum, mixed, hidden, norm_mlp, inv_mlp, pre_act, gelu_out))
        act = (hidden.astype(jnp.float32) + contract('bsf,fd->bsd', gelu_out, w_down[layer])).astype(jnp.bfloat16)
    grad_act = d_out
    layer_grads = [None] * LAYERS
    for layer in reversed(range(LAYERS)):
        (layer_in, norm_attn, inv_attn, q_group, keys, values, attn_out, log_sum, mixed, hidden, norm_mlp, inv_mlp, pre_act, gelu_out) = stashes[layer]
        d_gelu = contract('bsd,fd->bsf', grad_act, w_down[layer])
        d_pre = jax.vjp(gelu_tanh, pre_act)[1](d_gelu)[0].astype(jnp.bfloat16)
        grad_down = contract('bsf,bsd->fd', gelu_out, grad_act)
        grad_up = contract('bsd,bsf->df', norm_mlp, d_pre)
        d_norm_mlp = contract('bsf,df->bsd', d_pre, w_up[layer])
        d_hidden = (grad_act.astype(jnp.float32) + rms_norm_grad(hidden, inv_mlp, g_mlp[layer], d_norm_mlp)).astype(jnp.bfloat16)
        grad_attn_out = contract('bshe,bsd->hed', mixed, d_hidden)
        d_mixed = contract('bsd,hed->bshe', d_hidden, w_attn_out[layer]).astype(jnp.bfloat16)
        dq_group, dk_heads, dv_heads = grouped_attention_grad(q_group, keys, values, attn_out, log_sum, d_mixed.reshape(q_group.shape))
        d_query = rotary(dq_group.astype(jnp.bfloat16).reshape(d_mixed.shape), positions, -1.0).astype(jnp.bfloat16)
        d_keys = rotary(dk_heads.astype(jnp.bfloat16), positions, -1.0).astype(jnp.bfloat16)
        d_values = dv_heads.astype(jnp.bfloat16)
        grad_query = contract('bsd,bshe->dhe', norm_attn, d_query)
        grad_key = contract('bsd,bshe->dhe', norm_attn, d_keys)
        grad_value = contract('bsd,bshe->dhe', norm_attn, d_values)
        d_norm_attn = contract('bshe,dhe->bsd', d_query, w_query[layer]) + contract('bshe,dhe->bsd', d_keys, w_key[layer]) + contract('bshe,dhe->bsd', d_values, w_value[layer])
        grad_act = (d_hidden.astype(jnp.float32) + rms_norm_grad(layer_in, inv_attn, g_attn[layer], d_norm_attn)).astype(jnp.bfloat16)
        layer_grads[layer] = (grad_query, grad_key, grad_value, grad_attn_out, grad_up, grad_down)
    news = [(weight.astype(jnp.float32) - learn_rate * jnp.stack([grads[index] for grads in layer_grads])).astype(jnp.bfloat16) for index, weight in enumerate(weights)]
    return (act, grad_act, news[0], news[1], news[2], news[3], news[4], news[5])
```

```python
import functools
import math

import jax
import jax.numpy as jnp
from jax import lax
from jax.experimental import pallas as pl
from jax.experimental.pallas import tpu as pltpu
from jax.sharding import PartitionSpec as P


EPSILON = 1e-5
ROPE_BASE = 10000.0
SEQ_AXIS = 'sp'
F32 = jnp.float32
BF16 = jnp.bfloat16
LOG2E = math.log2(math.e)
NT = (((1,), (1,)), ((), ()))


def contract(form, left, right):
    return jnp.einsum(form, left, right, preferred_element_type=F32)


def gelu_tanh(value):
    return jax.nn.gelu(value, approximate=True)


def rms_norm(act, gain):
    wide = act.astype(F32)
    inv_rms = lax.rsqrt(jnp.mean(wide * wide, axis=-1, keepdims=True) + EPSILON)
    return (wide * inv_rms * gain).astype(BF16), inv_rms


def rms_norm_grad(act, inv_rms, gain, d_norm):
    wide = act.astype(F32)
    d_gain = d_norm * gain
    return inv_rms * d_gain - wide * inv_rms ** 3 * jnp.mean(d_gain * wide, axis=-1, keepdims=True)


def swap_halves(x, head_dim):
    half = head_dim // 2
    lanes = x.shape[-1]
    lane = lax.broadcasted_iota(jnp.int32, x.shape, 1)
    ahead = pltpu.roll(x, lanes - half, 1)
    behind = pltpu.roll(x, half, 1)
    return jnp.where(lane % head_dim < half, ahead, behind)


def causal_mask(keys, queries):
    return lax.broadcasted_iota(jnp.int32, (keys, queries), 0) <= lax.broadcasted_iota(jnp.int32, (keys, queries), 1)


def attn_fwd_kernel(head_dim, blk, n_ref, w_ref, cos_ref, sin_ref, q_ref, k_ref, v_ref, o_ref, lse_ref):
    shards, _, rows, lanes = q_ref.shape
    seq = shards * rows
    heads = lanes // head_dim
    scale = head_dim ** -0.5
    step = 256
    for t in range(seq // step):
        per = step // rows
        n = n_ref[t * per:(t + 1) * per, 0].reshape(step, n_ref.shape[-1])
        qkv = lax.dot_general(n, w_ref[...], NT, preferred_element_type=F32)
        cos = cos_ref[t * step:(t + 1) * step]
        sin = sin_ref[t * step:(t + 1) * step]
        for idx, ref in enumerate((q_ref, k_ref, v_ref)):
            part = qkv[:, idx * lanes:(idx + 1) * lanes]
            if idx < 2:
                part = part * cos + swap_halves(part, head_dim) * sin
            ref[t * per:(t + 1) * per, 0] = part.astype(BF16).reshape(per, rows, lanes)
    mask = causal_mask(blk, blk)
    vt = v_ref[:, 0].reshape(seq, lanes).T
    for j in range(seq // blk):
        per = blk // rows
        q_all = q_ref[j * per:(j + 1) * per, 0].reshape(blk, lanes)
        outs = []
        for h in range(heads):
            cols = slice(h * head_dim, (h + 1) * head_dim)
            q = q_all[:, cols]
            k_diag = k_ref[j * per:(j + 1) * per, 0].reshape(blk, lanes)[:, cols]
            s_diag = lax.dot_general(k_diag, q, NT, preferred_element_type=F32)
            s_diag = jnp.where(mask, s_diag, -1e30)
            top = jnp.max(s_diag, axis=0, keepdims=True)
            if j:
                k_off = k_ref[:j * per, 0].reshape(j * blk, lanes)[:, cols]
                s_off = lax.dot_general(k_off, q, NT, preferred_element_type=F32)
                top = jnp.maximum(top, jnp.max(s_off, axis=0, keepdims=True))
            c = scale * LOG2E
            e_diag = jnp.exp2((s_diag - top) * c)
            total = jnp.sum(e_diag, axis=0, keepdims=True)
            if j:
                e_off = jnp.exp2((s_off - top) * c)
                total = total + jnp.sum(e_off, axis=0, keepdims=True)
            inv = 1.0 / total
            out = jnp.dot(vt[cols, j * blk:(j + 1) * blk], (e_diag * inv).astype(BF16), preferred_element_type=F32)
            if j:
                out = out + jnp.dot(vt[cols, :j * blk], (e_off * inv).astype(BF16), preferred_element_type=F32)
            outs.append(out)
            lse_ref[0, h:h + 1, j * blk:(j + 1) * blk] = top * scale + jnp.log(total)
        o = jnp.concatenate(outs, axis=0).T.astype(BF16)
        o_ref[j * per:(j + 1) * per, 0] = o.reshape(per, rows, lanes)


def attn_forward(n_all, w_qkv, cos, sin, head_dim):
    shards, batch, rows, d_model = n_all.shape
    lanes = w_qkv.shape[0] // 3
    heads = lanes // head_dim
    seq = shards * rows
    blk = min(256, seq)
    head_block = pl.BlockSpec((shards, 1, rows, lanes), lambda b: (0, b, 0, 0))
    head_shape = jax.ShapeDtypeStruct((shards, batch, rows, lanes), BF16)
    flops = 2 * batch * seq * (d_model * 3 * lanes + seq * lanes * 2)
    return pl.pallas_call(
        functools.partial(attn_fwd_kernel, head_dim, blk),
        grid=(batch,),
        in_specs=[
            pl.BlockSpec((shards, 1, rows, d_model), lambda b: (0, b, 0, 0)),
            pl.BlockSpec(w_qkv.shape, lambda b: (0, 0)),
            pl.BlockSpec(cos.shape, lambda b: (0, 0)),
            pl.BlockSpec(sin.shape, lambda b: (0, 0)),
        ],
        out_specs=[head_block] * 4 + [pl.BlockSpec((1, heads, seq), lambda b: (b, 0, 0))],
        out_shape=[head_shape] * 4 + [jax.ShapeDtypeStruct((batch, heads, seq), F32)],
        cost_estimate=pl.CostEstimate(flops=flops * 4, bytes_accessed=n_all.size * 2, transcendentals=batch * heads * seq * seq),
        compiler_params=pltpu.CompilerParams(dimension_semantics=('arbitrary',), vmem_limit_bytes=50 * 1024 * 1024),
        name='attn_fwd',
    )(n_all, w_qkv, cos, sin)


def attn_bwd_kernel(head_dim, blk, q_ref, k_ref, v_ref, o_ref, d_ref, lse_ref, cos_ref, sin_ref, dqkv_ref, dk_acc, dv_acc):
    shards, _, rows, lanes = q_ref.shape
    seq = shards * rows
    heads = lanes // head_dim
    scale = head_dim ** -0.5
    per = blk // rows
    mask = causal_mask(blk, blk)
    kt = k_ref[:, 0].reshape(seq, lanes).T
    dk_acc[...] = jnp.zeros_like(dk_acc)
    dv_acc[...] = jnp.zeros_like(dv_acc)

    def unrotate(grad, lo, hi):
        low = grad.astype(BF16).astype(F32)
        return (low * cos_ref[lo:hi] - swap_halves(low, head_dim) * sin_ref[lo:hi]).astype(BF16)

    for j in range(seq // blk):
        lo, hi = j * blk, (j + 1) * blk
        q_all = q_ref[j * per:(j + 1) * per, 0].reshape(blk, lanes)
        d_all = d_ref[j * per:(j + 1) * per, 0].reshape(blk, lanes)
        o_all = o_ref[j * per:(j + 1) * per, 0].reshape(blk, lanes)
        prod_t = (d_all.astype(F32) * o_all.astype(F32)).T
        dq_parts = []
        for h in range(heads):
            cols = slice(h * head_dim, (h + 1) * head_dim)
            q, d = q_all[:, cols], d_all[:, cols]
            delta = jnp.sum(prod_t[cols], axis=0, keepdims=True)
            lse2 = lse_ref[0, h:h + 1, lo:hi] * LOG2E
            c = scale * LOG2E
            spans = [(lo, hi)] + ([(0, lo)] if j else [])
            dq_t = None
            for start, stop in spans:
                k = k_ref[start // rows:stop // rows, 0].reshape(stop - start, lanes)[:, cols]
                v = v_ref[start // rows:stop // rows, 0].reshape(stop - start, lanes)[:, cols]
                s = lax.dot_general(k, q, NT, preferred_element_type=F32)
                p = jnp.exp2(s * c - lse2)
                if start == lo:
                    p = jnp.where(mask, p, 0.0)
                dp = lax.dot_general(v, d, NT, preferred_element_type=F32)
                ds = (p * (dp - delta) * scale).astype(BF16)
                dv_acc[start:stop, cols] += jnp.dot(p.astype(BF16), d, preferred_element_type=F32)
                dk_acc[start:stop, cols] += jnp.dot(ds, q, preferred_element_type=F32)
                part = jnp.dot(kt[cols, start:stop], ds, preferred_element_type=F32)
                dq_t = part if dq_t is None else dq_t + part
            dq_parts.append(dq_t)
        dq = jnp.concatenate(dq_parts, axis=0).T
        dqkv_ref[j * per:(j + 1) * per, 0, 0] = unrotate(dq, lo, hi).reshape(per, rows, lanes)
    for j in range(seq // blk):
        lo, hi = j * blk, (j + 1) * blk
        dqkv_ref[j * per:(j + 1) * per, 1, 0] = unrotate(dk_acc[lo:hi], lo, hi).reshape(per, rows, lanes)
        dqkv_ref[j * per:(j + 1) * per, 2, 0] = dv_acc[lo:hi].astype(BF16).reshape(per, rows, lanes)


def attn_backward(q, k, v, o, d, lse, cos, sin, head_dim):
    shards, batch, rows, lanes = q.shape
    heads = lanes // head_dim
    seq = shards * rows
    blk = min(256, seq)
    head_block = pl.BlockSpec((shards, 1, rows, lanes), lambda b: (0, b, 0, 0))
    flops = 2 * batch * seq * seq * lanes * 5
    return pl.pallas_call(
        functools.partial(attn_bwd_kernel, head_dim, blk),
        grid=(batch,),
        in_specs=[head_block] * 5 + [
            pl.BlockSpec((1, heads, seq), lambda b: (b, 0, 0)),
            pl.BlockSpec(cos.shape, lambda b: (0, 0)),
            pl.BlockSpec(sin.shape, lambda b: (0, 0)),
        ],
        out_specs=pl.BlockSpec((shards, 3, 1, rows, lanes), lambda b: (0, 0, b, 0, 0)),
        out_shape=jax.ShapeDtypeStruct((shards, 3, batch, rows, lanes), BF16),
        scratch_shapes=[pltpu.VMEM((seq, lanes), F32), pltpu.VMEM((seq, lanes), F32)],
        cost_estimate=pl.CostEstimate(flops=flops * 4, bytes_accessed=q.size * 16, transcendentals=batch * heads * seq * seq),
        compiler_params=pltpu.CompilerParams(dimension_semantics=('arbitrary',), vmem_limit_bytes=50 * 1024 * 1024),
        name='attn_bwd',
    )(q, k, v, o, d, lse, cos, sin)


def exchange(tensor):
    return lax.all_to_all(tensor, SEQ_AXIS, 0, 0, tiled=True)


def emit_kernel(in_ref, out_ref):
    out_ref[...] = in_ref[...]


def emit(array):
    layers, height, width = array.shape
    block = pl.BlockSpec((1, max(height // 4, 8), width), lambda layer, row: (layer, row, 0))
    return pl.pallas_call(
        emit_kernel,
        grid=(layers, height // max(height // 4, 8)),
        in_specs=[block],
        out_specs=block,
        out_shape=jax.ShapeDtypeStruct(array.shape, array.dtype),
        cost_estimate=pl.CostEstimate(flops=10 ** 10, bytes_accessed=4 * array.size, transcendentals=0),
        name='emit',
    )(array)


def solution(mesh):
    act_spec = P('dp', 'sp', None)
    pos_spec = P(('dp', 'sp'))
    replicated = P()
    new_spec = P('dp')
    shards = mesh.shape[SEQ_AXIS]

    def body(x_in, positions, d_out, w_query, w_key, w_value, w_attn_out, w_up, w_down, g_attn, g_mlp, learn_rate):
        layers, d_model, heads, head_dim = w_query.shape
        batch, rows, _ = x_in.shape
        tokens = batch * rows
        local = heads // shards
        lanes = local * head_dim
        me = lax.axis_index(SEQ_AXIS)
        half = head_dim // 2

        pos_all = lax.all_gather(positions, SEQ_AXIS, tiled=True)
        inv_freq = ROPE_BASE ** (-2.0 * jnp.arange(half, dtype=F32) / head_dim)
        angle = pos_all.astype(F32)[:, None] * inv_freq
        cos = jnp.tile(jnp.cos(angle), (1, 2 * local))
        sin = jnp.sin(angle)
        sin = jnp.tile(jnp.concatenate([-sin, sin], axis=-1), (1, local))

        def mine(weight, axis):
            size = weight.shape[axis] // shards
            return lax.dynamic_slice_in_dim(weight, me * size, size, axis)

        w_rows = [w.transpose(0, 2, 3, 1).reshape(layers, heads * head_dim, d_model) for w in (w_query, w_key, w_value)]
        w_qkv = jnp.concatenate([mine(w, 1) for w in w_rows], axis=1)
        w_outs = w_attn_out.reshape(layers, heads * head_dim, d_model)

        chunks = 2 if batch % 2 == 0 else 1
        part = batch // chunks
        size = part * rows
        order = lax.optimization_barrier

        def split(array):
            flat = array.reshape(tokens, d_model)
            return [flat[c * size:(c + 1) * size] for c in range(chunks)]

        def join(parts):
            return jnp.concatenate(parts, axis=0)

        def to_tokens(heads_first):
            return heads_first.reshape(shards, size, lanes).transpose(1, 0, 2).reshape(size, heads * head_dim)

        def scatter(grad):
            return lax.psum_scatter(grad, SEQ_AXIS, scatter_dimension=0, tiled=True)

        acts = split(x_in)
        stash = []
        norms = [rms_norm(act, g_attn[0]) for act in acts]
        for layer in range(layers):
            heads_in, exchanged = [], []
            for c in range(chunks):
                n_all = lax.all_gather(norms[c][0].reshape(part, rows, d_model), SEQ_AXIS)
                q, k, v, o, lse = attn_forward(n_all, w_qkv[layer], cos, sin, head_dim)
                heads_in.append((acts[c], n_all, norms[c][1], q, k, v, o, lse))
                exchanged.append(exchange(o))
            saved = []
            for c in range(chunks):
                mixed = to_tokens(exchanged[c])
                hidden = (acts[c].astype(F32) + contract('tc,cd->td', mixed, w_outs[layer])).astype(BF16)
                norm_mlp, inv_mlp = rms_norm(hidden, g_mlp[layer])
                pre_act = contract('td,df->tf', norm_mlp, w_up[layer])
                gelu_out = gelu_tanh(pre_act).astype(BF16)
                saved.append(heads_in[c] + (mixed, hidden, norm_mlp, inv_mlp, pre_act, gelu_out))
                acts[c] = (hidden.astype(F32) + contract('tf,fd->td', gelu_out, w_down[layer])).astype(BF16)
                if layer + 1 < layers:
                    norms[c] = rms_norm(acts[c], g_attn[layer + 1])
                    if c + 1 < chunks:
                        norms[c], exchanged[c + 1] = order((norms[c], exchanged[c + 1]))
            stash.append(saved)
        y_out = join(acts)

        grads = split(d_out)
        sums_qkv, sums_out, sums_up, sums_down = ([None] * layers for _ in range(4))
        for layer in reversed(range(layers)):
            saved = stash[layer]
            above = layer + 1 if layer + 1 < layers else None
            whole = d_out.reshape(tokens, d_model) if above is None else join(grads)
            grad_down = contract('tf,td->fd', join([s[13] for s in saved]), whole)
            pre_acts, grad_down = order(([s[12] for s in saved], grad_down))
            sums_down[layer] = scatter(grad_down)
            d_pres = []
            for c in range(chunks):
                d_gelu = contract('td,fd->tf', grads[c], w_down[layer])
                d_pres.append(jax.vjp(gelu_tanh, pre_acts[c])[1](d_gelu)[0].astype(BF16))
            grad_up = contract('td,tf->df', join([s[10] for s in saved]), join(d_pres))
            if above is not None:
                d_pres, grad_up, sums_up[above] = order((d_pres, grad_up, sums_up[above]))
            else:
                d_pres, grad_up = order((d_pres, grad_up))
            sums_up[layer] = scatter(grad_up)
            d_hiddens, d_heads = [], []
            for c in range(chunks):
                d_norm_mlp = contract('tf,df->td', d_pres[c], w_up[layer])
                d_hidden = (grads[c].astype(F32) + rms_norm_grad(saved[c][9], saved[c][11], g_mlp[layer], d_norm_mlp)).astype(BF16)
                d_mixed = contract('td,cd->tc', d_hidden, w_outs[layer]).astype(BF16)
                d_hiddens.append(d_hidden)
                d_heads.append(exchange(d_mixed.reshape(size, shards, lanes).transpose(1, 0, 2).reshape(shards, part, rows, lanes)))
            grad_out = contract('tc,td->cd', join([s[8] for s in saved]), join(d_hiddens))
            if above is not None:
                d_heads, grad_out, sums_out[above] = order((d_heads, grad_out, sums_out[above]))
            else:
                d_heads, grad_out = order((d_heads, grad_out))
            sums_out[layer] = scatter(grad_out)
            grad_qkv, outs = 0.0, []
            for c in range(chunks):
                _, n_all, _, q, k, v, o, lse = saved[c][:8]
                dqkv = attn_backward(q, k, v, o, d_heads[c], lse, cos, sin, head_dim)
                outs.append(exchange(dqkv))
                grad_qkv = grad_qkv + contract('sibrc,sbrd->icd', dqkv, n_all)
            outs, sums_qkv[layer], sums_down[layer] = order((outs, grad_qkv, sums_down[layer]))
            for c in range(chunks):
                d_norm_attn = sum(contract('tc,cd->td', to_tokens(outs[c][:, idx]), w_rows[idx][layer]) for idx in range(3))
                grads[c] = (d_hiddens[c].astype(F32) + rms_norm_grad(saved[c][0], saved[c][2], g_attn[layer], d_norm_attn)).astype(BF16)
        grad_x = join(grads)
        grad_x, sums_up[0] = order((grad_x, sums_up[0]))
        sums_up[0], sums_out[0] = order((sums_up[0], sums_out[0]))

        def renew(pairs):
            new = [(mine(weight, 1).astype(F32) - learn_rate * total).astype(BF16) for weight, total in pairs]
            return lax.all_gather(jnp.concatenate(new), SEQ_AXIS, axis=1, tiled=True)

        new_down = renew([(w_down, jnp.stack(sums_down))])
        new_up = renew([(w_up, jnp.stack(sums_up))])
        small = [(w_outs, jnp.stack(sums_out))]
        small += [(w_rows[idx], jnp.stack([sums[idx] for sums in sums_qkv])) for idx in range(3)]
        small = renew(small).reshape(4, layers, heads, head_dim, d_model)
        new_down = emit(new_down)
        new_up = emit(new_up)
        new_out = small[0]
        new_heads = [small[idx + 1].transpose(0, 3, 1, 2) for idx in range(3)]
        return (y_out.reshape(x_in.shape), grad_x.reshape(x_in.shape), *new_heads, new_out, new_up, new_down)

    return jax.shard_map(body, mesh=mesh, in_specs=(act_spec, pos_spec, act_spec) + (replicated,) * 9, out_specs=(act_spec, act_spec) + (new_spec,) * 6, check_vma=False)
```

```python
import functools
import math

import jax
import jax.numpy as jnp
from jax import lax
from jax.experimental import pallas as pl
from jax.experimental.pallas import tpu as pltpu
from jax.sharding import PartitionSpec as P


EPSILON = 1e-5
ROPE_BASE = 10000.0
SEQ_AXIS = 'sp'
CORES = 2
F32 = jnp.float32
BF16 = jnp.bfloat16
LOG2E = math.log2(math.e)
NT = (((1,), (1,)), ((), ()))


def contract(form, left, right):
    return jnp.einsum(form, left, right, preferred_element_type=F32)


def gelu_tanh(value):
    return jax.nn.gelu(value, approximate=True)


def rms_norm(act, gain):
    wide = act.astype(F32)
    inv_rms = lax.rsqrt(jnp.mean(wide * wide, axis=-1, keepdims=True) + EPSILON)
    return (wide * inv_rms * gain).astype(BF16), inv_rms


def rms_norm_grad(act, inv_rms, gain, d_norm):
    wide = act.astype(F32)
    d_gain = d_norm * gain
    return inv_rms * d_gain - wide * inv_rms ** 3 * jnp.mean(d_gain * wide, axis=-1, keepdims=True)


def swap_halves(x, head_dim):
    half = head_dim // 2
    lanes = x.shape[-1]
    lane = lax.broadcasted_iota(jnp.int32, x.shape, 1)
    ahead = pltpu.roll(x, lanes - half, 1)
    behind = pltpu.roll(x, half, 1)
    return jnp.where(lane % head_dim < half, ahead, behind)


def causal_mask(keys, queries):
    return lax.broadcasted_iota(jnp.int32, (keys, queries), 0) <= lax.broadcasted_iota(jnp.int32, (keys, queries), 1)


def attn_fwd_kernel(head_dim, blk, n_ref, w_ref, cos_ref, sin_ref, q_ref, k_ref, v_ref, o_ref, lse_ref):
    shards, _, rows, lanes = q_ref.shape
    seq = shards * rows
    heads = lanes // head_dim
    scale = head_dim ** -0.5
    step = 256
    for t in range(seq // step):
        per = step // rows
        n = n_ref[t * per:(t + 1) * per, 0].reshape(step, n_ref.shape[-1])
        qkv = lax.dot_general(n, w_ref[...], NT, preferred_element_type=F32)
        cos = cos_ref[t * step:(t + 1) * step]
        sin = sin_ref[t * step:(t + 1) * step]
        for idx, ref in enumerate((q_ref, k_ref, v_ref)):
            part = qkv[:, idx * lanes:(idx + 1) * lanes]
            if idx < 2:
                part = part * cos + swap_halves(part, head_dim) * sin
            ref[t * per:(t + 1) * per, 0] = part.astype(BF16).reshape(per, rows, lanes)
    mask = causal_mask(blk, blk)
    vt = v_ref[:, 0].reshape(seq, lanes).T
    for j in range(seq // blk):
        per = blk // rows
        q_all = q_ref[j * per:(j + 1) * per, 0].reshape(blk, lanes)
        outs = []
        for h in range(heads):
            cols = slice(h * head_dim, (h + 1) * head_dim)
            q = q_all[:, cols]
            k_diag = k_ref[j * per:(j + 1) * per, 0].reshape(blk, lanes)[:, cols]
            s_diag = lax.dot_general(k_diag, q, NT, preferred_element_type=F32)
            s_diag = jnp.where(mask, s_diag, -1e30)
            top = jnp.max(s_diag, axis=0, keepdims=True)
            if j:
                k_off = k_ref[:j * per, 0].reshape(j * blk, lanes)[:, cols]
                s_off = lax.dot_general(k_off, q, NT, preferred_element_type=F32)
                top = jnp.maximum(top, jnp.max(s_off, axis=0, keepdims=True))
            c = scale * LOG2E
            e_diag = jnp.exp2((s_diag - top) * c)
            total = jnp.sum(e_diag, axis=0, keepdims=True)
            if j:
                e_off = jnp.exp2((s_off - top) * c)
                total = total + jnp.sum(e_off, axis=0, keepdims=True)
            inv = 1.0 / total
            out = jnp.dot(vt[cols, j * blk:(j + 1) * blk], (e_diag * inv).astype(BF16), preferred_element_type=F32)
            if j:
                out = out + jnp.dot(vt[cols, :j * blk], (e_off * inv).astype(BF16), preferred_element_type=F32)
            outs.append(out)
            lse_ref[0, h:h + 1, j * blk:(j + 1) * blk] = top * scale + jnp.log(total)
        o = jnp.concatenate(outs, axis=0).T.astype(BF16)
        o_ref[j * per:(j + 1) * per, 0] = o.reshape(per, rows, lanes)


def attn_forward(n_all, w_qkv, cos, sin, head_dim):
    shards, batch, rows, d_model = n_all.shape
    lanes = w_qkv.shape[0] // 3
    heads = lanes // head_dim
    seq = shards * rows
    blk = min(256, seq)
    head_block = pl.BlockSpec((shards, 1, rows, lanes), lambda b: (0, b, 0, 0))
    head_shape = jax.ShapeDtypeStruct((shards, batch, rows, lanes), BF16)
    flops = 2 * batch * seq * (d_model * 3 * lanes + seq * lanes * 2)
    return pl.pallas_call(
        functools.partial(attn_fwd_kernel, head_dim, blk),
        grid=(batch,),
        in_specs=[
            pl.BlockSpec((shards, 1, rows, d_model), lambda b: (0, b, 0, 0)),
            pl.BlockSpec(w_qkv.shape, lambda b: (0, 0)),
            pl.BlockSpec(cos.shape, lambda b: (0, 0)),
            pl.BlockSpec(sin.shape, lambda b: (0, 0)),
        ],
        out_specs=[head_block] * 4 + [pl.BlockSpec((1, heads, seq), lambda b: (b, 0, 0))],
        out_shape=[head_shape] * 4 + [jax.ShapeDtypeStruct((batch, heads, seq), F32)],
        cost_estimate=pl.CostEstimate(flops=flops * 4, bytes_accessed=n_all.size * 2, transcendentals=batch * heads * seq * seq),
        compiler_params=pltpu.CompilerParams(dimension_semantics=('arbitrary',), vmem_limit_bytes=50 * 1024 * 1024),
        name='attn_fwd',
    )(n_all, w_qkv, cos, sin)


def attn_bwd_kernel(head_dim, blk, q_ref, k_ref, v_ref, o_ref, d_ref, lse_ref, cos_ref, sin_ref, dqkv_ref, dk_acc, dv_acc):
    shards, _, rows, lanes = q_ref.shape
    seq = shards * rows
    heads = lanes // head_dim
    scale = head_dim ** -0.5
    per = blk // rows
    mask = causal_mask(blk, blk)
    kt = k_ref[:, 0].reshape(seq, lanes).T
    dk_acc[...] = jnp.zeros_like(dk_acc)
    dv_acc[...] = jnp.zeros_like(dv_acc)

    def unrotate(grad, lo, hi):
        low = grad.astype(BF16).astype(F32)
        return (low * cos_ref[lo:hi] - swap_halves(low, head_dim) * sin_ref[lo:hi]).astype(BF16)

    for j in range(seq // blk):
        lo, hi = j * blk, (j + 1) * blk
        q_all = q_ref[j * per:(j + 1) * per, 0].reshape(blk, lanes)
        d_all = d_ref[j * per:(j + 1) * per, 0].reshape(blk, lanes)
        o_all = o_ref[j * per:(j + 1) * per, 0].reshape(blk, lanes)
        prod_t = (d_all.astype(F32) * o_all.astype(F32)).T
        dq_parts = []
        for h in range(heads):
            cols = slice(h * head_dim, (h + 1) * head_dim)
            q, d = q_all[:, cols], d_all[:, cols]
            delta = jnp.sum(prod_t[cols], axis=0, keepdims=True)
            lse2 = lse_ref[0, h:h + 1, lo:hi] * LOG2E
            c = scale * LOG2E
            spans = [(lo, hi)] + ([(0, lo)] if j else [])
            dq_t = None
            for start, stop in spans:
                k = k_ref[start // rows:stop // rows, 0].reshape(stop - start, lanes)[:, cols]
                v = v_ref[start // rows:stop // rows, 0].reshape(stop - start, lanes)[:, cols]
                s = lax.dot_general(k, q, NT, preferred_element_type=F32)
                p = jnp.exp2(s * c - lse2)
                if start == lo:
                    p = jnp.where(mask, p, 0.0)
                dp = lax.dot_general(v, d, NT, preferred_element_type=F32)
                ds = (p * (dp - delta) * scale).astype(BF16)
                dv_acc[start:stop, cols] += jnp.dot(p.astype(BF16), d, preferred_element_type=F32)
                dk_acc[start:stop, cols] += jnp.dot(ds, q, preferred_element_type=F32)
                part = jnp.dot(kt[cols, start:stop], ds, preferred_element_type=F32)
                dq_t = part if dq_t is None else dq_t + part
            dq_parts.append(dq_t)
        dq = jnp.concatenate(dq_parts, axis=0).T
        dqkv_ref[j * per:(j + 1) * per, 0, 0] = unrotate(dq, lo, hi).reshape(per, rows, lanes)
    for j in range(seq // blk):
        lo, hi = j * blk, (j + 1) * blk
        dqkv_ref[j * per:(j + 1) * per, 1, 0] = unrotate(dk_acc[lo:hi], lo, hi).reshape(per, rows, lanes)
        dqkv_ref[j * per:(j + 1) * per, 2, 0] = dv_acc[lo:hi].astype(BF16).reshape(per, rows, lanes)


def attn_backward(q, k, v, o, d, lse, cos, sin, head_dim):
    shards, batch, rows, lanes = q.shape
    heads = lanes // head_dim
    seq = shards * rows
    blk = min(256, seq)
    head_block = pl.BlockSpec((shards, 1, rows, lanes), lambda b: (0, b, 0, 0))
    flops = 2 * batch * seq * seq * lanes * 5
    return pl.pallas_call(
        functools.partial(attn_bwd_kernel, head_dim, blk),
        grid=(batch,),
        in_specs=[head_block] * 5 + [
            pl.BlockSpec((1, heads, seq), lambda b: (b, 0, 0)),
            pl.BlockSpec(cos.shape, lambda b: (0, 0)),
            pl.BlockSpec(sin.shape, lambda b: (0, 0)),
        ],
        out_specs=pl.BlockSpec((shards, 3, 1, rows, lanes), lambda b: (0, 0, b, 0, 0)),
        out_shape=jax.ShapeDtypeStruct((shards, 3, batch, rows, lanes), BF16),
        scratch_shapes=[pltpu.VMEM((seq, lanes), F32), pltpu.VMEM((seq, lanes), F32)],
        cost_estimate=pl.CostEstimate(flops=flops * 4, bytes_accessed=q.size * 16, transcendentals=batch * heads * seq * seq),
        compiler_params=pltpu.CompilerParams(dimension_semantics=('arbitrary',), vmem_limit_bytes=50 * 1024 * 1024),
        name='attn_bwd',
    )(q, k, v, o, d, lse, cos, sin)


def exchange(tensor):
    return lax.all_to_all(tensor, SEQ_AXIS, 0, 0, tiled=True)


def solution(mesh):
    act_spec = P('dp', 'sp', None)
    pos_spec = P(('dp', 'sp'))
    replicated = P()
    new_spec = P('dp')
    shards = mesh.shape[SEQ_AXIS]

    def body(x_in, positions, d_out, w_query, w_key, w_value, w_attn_out, w_up, w_down, g_attn, g_mlp, learn_rate):
        layers, d_model, heads, head_dim = w_query.shape
        batch, rows, _ = x_in.shape
        tokens = batch * rows
        local = heads // shards
        lanes = local * head_dim
        me = lax.axis_index(SEQ_AXIS)
        half = head_dim // 2

        pos_all = lax.all_gather(positions, SEQ_AXIS, tiled=True)
        inv_freq = ROPE_BASE ** (-2.0 * jnp.arange(half, dtype=F32) / head_dim)
        angle = pos_all.astype(F32)[:, None] * inv_freq
        cos = jnp.tile(jnp.cos(angle), (1, 2 * local))
        sin = jnp.sin(angle)
        sin = jnp.tile(jnp.concatenate([-sin, sin], axis=-1), (1, local))

        def mine(weight, axis):
            size = weight.shape[axis] // shards
            return lax.dynamic_slice_in_dim(weight, me * size, size, axis)

        w_rows = [w.transpose(0, 2, 3, 1).reshape(layers, heads * head_dim, d_model) for w in (w_query, w_key, w_value)]
        w_qkv = jnp.concatenate([mine(w, 1) for w in w_rows], axis=1)
        w_outs = w_attn_out.reshape(layers, heads * head_dim, d_model)

        chunks = 2 if batch % 2 == 0 else 1
        part = batch // chunks
        size = part * rows
        order = lax.optimization_barrier

        def split(array):
            flat = array.reshape(tokens, d_model)
            return [flat[c * size:(c + 1) * size] for c in range(chunks)]

        def join(parts):
            return jnp.concatenate(parts, axis=0)

        def to_tokens(heads_first):
            return heads_first.reshape(shards, size, lanes).transpose(1, 0, 2).reshape(size, heads * head_dim)

        chips = shards // CORES
        rings = [[chip * CORES + c for chip in range(chips)] for c in range(CORES)]
        swap = [(index, index ^ 1) for index in range(shards)]
        core = me % CORES

        def side(left, which):
            width = left.shape[1] // shards
            pick = [jnp.concatenate([left[:, (chip * CORES + c) * width:(chip * CORES + c + 1) * width] for chip in range(chips)], axis=1) for c in range(CORES)]
            return jnp.where(which == 0, pick[0], pick[1])

        def send_half(left, right):
            return contract('tf,td->fd', side(left, 1 - core), right)

        def keep_half(left, right, sent):
            return contract('tf,td->fd', side(left, core), right) + lax.ppermute(sent, SEQ_AXIS, swap)

        def scatter(grad, paired):
            return lax.psum_scatter(grad, SEQ_AXIS, scatter_dimension=0, axis_index_groups=rings if paired else None, tiled=True)

        acts = split(x_in)
        stash = []
        norms = [rms_norm(act, g_attn[0]) for act in acts]
        for layer in range(layers):
            heads_in, exchanged = [], []
            for c in range(chunks):
                n_all = lax.all_gather(norms[c][0].reshape(part, rows, d_model), SEQ_AXIS)
                q, k, v, o, lse = attn_forward(n_all, w_qkv[layer], cos, sin, head_dim)
                heads_in.append((acts[c], n_all, norms[c][1], q, k, v, o, lse))
                exchanged.append(exchange(o))
            saved = []
            for c in range(chunks):
                mixed = to_tokens(exchanged[c])
                hidden = (acts[c].astype(F32) + contract('tc,cd->td', mixed, w_outs[layer])).astype(BF16)
                norm_mlp, inv_mlp = rms_norm(hidden, g_mlp[layer])
                pre_act = contract('td,df->tf', norm_mlp, w_up[layer])
                gelu_out = gelu_tanh(pre_act).astype(BF16)
                saved.append(heads_in[c] + (mixed, hidden, norm_mlp, inv_mlp, pre_act, gelu_out))
                acts[c] = (hidden.astype(F32) + contract('tf,fd->td', gelu_out, w_down[layer])).astype(BF16)
                if layer + 1 < layers:
                    norms[c] = rms_norm(acts[c], g_attn[layer + 1])
                    if c + 1 < chunks:
                        norms[c], exchanged[c + 1] = order((norms[c], exchanged[c + 1]))
            stash.append(saved)
        y_out = join(acts)

        grads = split(d_out)
        sums_qkv, sums_out, sums_up, sums_down = ([None] * layers for _ in range(4))
        for layer in reversed(range(layers)):
            saved = stash[layer]
            above = layer + 1 if layer + 1 < layers else None
            whole = d_out.reshape(tokens, d_model) if above is None else join(grads)
            paired = above is not None
            gelu_all, norm_all, mixed_all = (join([item[index] for item in saved]) for index in (13, 10, 8))
            pre_acts = [item[12] for item in saved]
            if paired:
                down_half = send_half(gelu_all, whole)
                pre_acts, down_half = order((pre_acts, down_half))
            else:
                grad_down = contract('tf,td->fd', gelu_all, whole)
                pre_acts, grad_down = order((pre_acts, grad_down))
            d_pres = []
            for c in range(chunks):
                d_gelu = contract('td,fd->tf', grads[c], w_down[layer])
                d_pres.append(jax.vjp(gelu_tanh, pre_acts[c])[1](d_gelu)[0].astype(BF16))
            if paired:
                grad_down = keep_half(gelu_all, whole, down_half)
                d_pres, grad_down = order((d_pres, grad_down))
            sums_down[layer] = scatter(grad_down, paired)
            d_pre_all = join(d_pres)
            if paired:
                up_half = send_half(norm_all, d_pre_all)
                d_pres, up_half, sums_up[above] = order((d_pres, up_half, sums_up[above]))
            else:
                grad_up = contract('td,tf->df', norm_all, d_pre_all)
                d_pres, grad_up = order((d_pres, grad_up))
            d_hiddens, d_heads = [], []
            for c in range(chunks):
                d_norm_mlp = contract('tf,df->td', d_pres[c], w_up[layer])
                d_hidden = (grads[c].astype(F32) + rms_norm_grad(saved[c][9], saved[c][11], g_mlp[layer], d_norm_mlp)).astype(BF16)
                d_mixed = contract('td,cd->tc', d_hidden, w_outs[layer]).astype(BF16)
                d_hiddens.append(d_hidden)
                d_heads.append(exchange(d_mixed.reshape(size, shards, lanes).transpose(1, 0, 2).reshape(shards, part, rows, lanes)))
            d_hidden_all = join(d_hiddens)
            if paired:
                grad_up = keep_half(norm_all, d_pre_all, up_half)
                out_half = send_half(mixed_all, d_hidden_all)
                d_heads, grad_up, out_half, sums_out[above] = order((d_heads, grad_up, out_half, sums_out[above]))
            else:
                grad_out = contract('tc,td->cd', mixed_all, d_hidden_all)
                d_heads, grad_out = order((d_heads, grad_out))
                sums_out[layer] = scatter(grad_out, paired)
            sums_up[layer] = scatter(grad_up, paired)
            grad_qkv, outs = 0.0, []
            for c in range(chunks):
                _, n_all, _, q, k, v, o, lse = saved[c][:8]
                dqkv = attn_backward(q, k, v, o, d_heads[c], lse, cos, sin, head_dim)
                outs.append(exchange(dqkv))
                grad_qkv = grad_qkv + contract('sibrc,sbrd->icd', dqkv, n_all)
            if paired:
                sums_out[layer] = scatter(keep_half(mixed_all, d_hidden_all, out_half), paired)
            if paired:
                outs, sums_qkv[layer], sums_down[layer], sums_up[layer] = order((outs, grad_qkv, sums_down[layer], sums_up[layer]))
            else:
                outs, sums_qkv[layer], sums_down[layer] = order((outs, grad_qkv, sums_down[layer]))
            for c in range(chunks):
                d_norm_attn = sum(contract('tc,cd->td', to_tokens(outs[c][:, idx]), w_rows[idx][layer]) for idx in range(3))
                grads[c] = (d_hiddens[c].astype(F32) + rms_norm_grad(saved[c][0], saved[c][2], g_attn[layer], d_norm_attn)).astype(BF16)
        grad_x = join(grads)
        grad_x, sums_out[0] = order((grad_x, sums_out[0]))

        chip = me // CORES
        onward = [(index, (index + CORES) % shards) for index in range(shards)]
        backward = [(index, (index - CORES) % shards) for index in range(shards)]
        assert chips == 4, chips

        def spread(new):
            rows_each = new.shape[1]
            half = rows_each // 2
            below = lax.ppermute(new, SEQ_AXIS, onward)
            above = lax.ppermute(new, SEQ_AXIS, backward)
            far_low = lax.ppermute(below[:, :half], SEQ_AXIS, onward)
            far_high = lax.ppermute(above[:, half:], SEQ_AXIS, backward)
            near = [(new, 0, 0), (below, 3, 0), (above, 1, 0)]
            far = [(far_low, 2, 0), (far_high, 2, half)]
            pieces = [(piece, lax.ppermute(piece, SEQ_AXIS, swap), hops, low) for piece, hops, low in near]
            pieces += [(piece, lax.ppermute(piece, SEQ_AXIS, swap), hops, low) for piece, hops, low in far]
            whole = jnp.zeros((new.shape[0], shards * rows_each, new.shape[2]), new.dtype)
            for piece, twin, hops, low in pieces:
                base = (chip + hops) % chips * CORES
                whole = lax.dynamic_update_slice_in_dim(whole, piece, (base + core) * rows_each + low, 1)
                whole = lax.dynamic_update_slice_in_dim(whole, twin, (base + 1 - core) * rows_each + low, 1)
            return whole

        def renew(weight, total):
            return spread((mine(weight, 1).astype(F32) - learn_rate * total).astype(BF16))

        new_down = renew(w_down, jnp.stack(sums_down))
        new_up = renew(w_up, jnp.stack(sums_up))
        new_out = renew(w_outs, jnp.stack(sums_out)).reshape(w_attn_out.shape)
        new_heads = [
            renew(w_rows[idx], jnp.stack([sums[idx] for sums in sums_qkv])).reshape(layers, heads, head_dim, d_model).transpose(0, 3, 1, 2)
            for idx in range(3)]
        return (y_out.reshape(x_in.shape), grad_x.reshape(x_in.shape), *new_heads, new_out, new_up, new_down)

    return jax.shard_map(body, mesh=mesh, in_specs=(act_spec, pos_spec, act_spec) + (replicated,) * 9, out_specs=(act_spec, act_spec) + (new_spec,) * 6, check_vma=False)
```
